32 devices in a mesh: wide: 16 (over z, y, x), tall: 2 (over core).
Axes of the slice: x: 2, y: 2, z: 4, core: 2. Of those that a mesh axis runs over, the one named last changes fastest.
Arguments:
- tokens: bfloat16 [48, 384, 512], P('tall', 'wide'), may hold values from -6 to 6
- qkv_weight: bfloat16 [512, 1536], replicated, may hold values from -0.25 to 0.25
- proj_weight: bfloat16 [512, 512], replicated, may hold values from -0.25 to 0.25
- head_scale: float32 [16], replicated, may hold values from 5 to 100
- attn_gain: float32 [512], replicated, may hold values from 0.5 to 1.5
- router: bfloat16 [512, 16], replicated, may hold values from -0.25 to 0.25
- expert_in: bfloat16 [16, 512, 2048], P('wide', None, 'tall'), may hold values from -0.25 to 0.25
- expert_out: bfloat16 [16, 2048, 512], P('wide', 'tall'), may hold values from -0.125 to 0.125
- moe_gain: float32 [512], replicated, may hold values from 0.5 to 1.5
- expert_ids: int32 [2, 16, 576, 1], P('tall', 'wide'), may hold values from 0 to 15; in each aligned block of 576 rows (0 to 575, 576 to 1151, ..., all dimensions but the last counted through in order) at most 54 rows name the same one
- keep: int32 [2, 16, 576], P('tall', 'wide'), may hold values 0 or 1
Outputs:
- mixed: bfloat16 [48, 384, 512], P('tall', 'wide')
The draws below stay inside these ranges and needn't reach their ends.
Inputs may be any that keep to these rules, and one draw needn't show every extreme that they name: `expert_ids`: within the tokens of one tile (one index of the first two dimensions), no expert is named more than 54 times, a bound that some block reaches.
All inputs are finite; a program needn't handle non-finite values. No bound on the sum of `keep` on one device may be relied on, other than what follows from the above.
Results may differ from the reference program's by a relative error of at most 0.012.
The reference program's roundings to bfloat16 on the way count: a program that leaves them out, or rounds other values in their place, can miss the bound.
Values may be sent and summed in bfloat16 or wider, within the bound.
No kernel may reach another device: no remote copies, remote signals or barrier semaphores. Data moves between devices by JAX's collectives and lax.ppermute only.
A program may use at most 64 MiB of HBM per device.

```python
import math
import jax
import jax.numpy as jnp
import numpy as np
from jax import lax

D = 512
HEADS = 16
HID = 2048
WIN = 24
TILE_H = 24
HEAD_DIM = 32
SHIFT = 12
TOK_DEV = 576
NH = 48
NW = 384
EXPERTS = 16
CAP = 54
N_WIDE = 16
N_TALL = 2


def plant(values, key, least, high):
    extent = values.shape
    place = [jax.random.randint(jax.random.fold_in(key, axis), (), 0, extent[axis]) for axis in range(len(extent))]
    values = values.at[tuple(place)].set(least)
    longest = extent.index(max(extent))
    place[longest] = (place[longest] + 1) % extent[longest]
    return values.at[tuple(place)].set(high)


def shard_levels(key, extent, split, smallest, high):
    level, own = 1.0, jax.random.fold_in(key, 6)
    for position, parts in split:
        draws = jnp.exp(jax.random.uniform(jax.random.fold_in(own, position), (parts,), jnp.float32, smallest / len(split), high / len(split)))
        level = level * jnp.repeat(draws, extent[position] // parts).reshape([-1 if axis == position else 1 for axis in range(len(extent))])
    return level


def shared_out(own_key, own, number, rows, number_of, top, bound, lean):
    order = jax.random.permutation(own_key, number_of)
    crowded, ordinary = load_shares(number_of, rows * top, bound, lean, True), load_shares(number_of, rows * top, bound, lean, False)
    places = jnp.arange(number_of)

    def named(lengths, offset_by):
        used = int((lengths > 0).sum())
        fixed = max(1, used // 4)
        passed = fixed + (places - fixed + offset_by * (used - fixed)) % max(1, number_of - fixed)
        return jnp.zeros((number_of,), jnp.int32).at[order[jnp.where(places < fixed, places, passed)]].set(jnp.asarray(lengths, jnp.int32))

    lengths = jnp.where(number % 4 == 0, named(crowded, number // 4), named(ordinary, number - number // 4 - 1))
    mixed = jax.random.permutation(jax.random.fold_in(own, 3), number_of)
    source_of, receiver = mixed[0:number_of // 2 * 2:2], mixed[1:number_of // 2 * 2:2]
    margin = jnp.minimum(lengths[source_of] - 1, bound - lengths[receiver]) // 2
    margin = jnp.where((source_of == order[0]) | (receiver == order[0]) | (lengths[receiver] == 0), 0, jnp.maximum(margin, 0))
    passed = jax.random.randint(jax.random.fold_in(own, 4), (number_of // 2,), 0, 1 << 20) % (margin + 1)
    lengths = lengths.at[source_of].add(-passed).at[receiver].add(passed)
    items = jnp.searchsorted(jnp.cumsum(lengths), jnp.arange(rows * top), side="right").astype(jnp.int32)
    listing = items.reshape(top, rows).T
    listing = listing[jax.random.permutation(jax.random.fold_in(own, 1), rows)]
    offset_by = jax.random.randint(jax.random.fold_in(own, 2), (rows, 1), 0, top)
    return jnp.take_along_axis(listing, (jnp.arange(top)[None, :] + offset_by) % top, axis=1)


def load_shares(amount, total, most, lean, full):
    portions = [(1 << 20) // math.isqrt(grade ** lean) + 1 for grade in range(1, amount + 1)]
    largest = most if full else min(most, max(-(-total // amount), total * portions[0] // sum(portions)))
    least = 1 if total - largest >= amount - 1 else 0
    given, surplus = [largest] + [least] * (amount - 1), total - largest - least * (amount - 1)
    while surplus > 0:
        candidates = [i for i in range(1, amount) if given[i] < largest] or [i for i in range(1, amount) if given[i] < most]
        mass, remaining = sum([portions[i] for i in candidates]), surplus
        for i in candidates:
            more = min(most - given[i], max(1, remaining * portions[i] // mass), surplus)
            given[i] = given[i] + more
            surplus = surplus - more
    return np.array(given)


def normal_values(stream_key, extent, scale, most, shards=(), held_as=jnp.bfloat16):
    drawn = scale * jax.random.normal(stream_key, extent, jnp.float32)
    if shards:
        drawn = drawn * shard_levels(stream_key, extent, shards, -0.22, 0.18)
    return jnp.clip(drawn, -most, most).astype(held_as)


def setup_inputs(seed: int = 0) -> dict:
    arg_keys = jax.random.split(jax.random.key(seed), 12)
    tokens = normal_values(arg_keys[0], (NH, NW, D), 1.0, 6.0, ((0, 2), (1, 16)))
    qkv_weight = normal_values(arg_keys[1], (D, 3 * D), D ** -0.5, 0.25)
    proj_weight = normal_values(arg_keys[2], (D, D), D ** -0.5, 0.25)
    head_scale = jnp.clip(jnp.exp(jax.random.uniform(arg_keys[3], (HEADS,), jnp.float32, math.log(5.0), math.log(100.0))), 5.0, 100.0)
    attn_gain = jnp.clip(1.0 + 0.1 * jax.random.normal(arg_keys[4], (D,), jnp.float32), 0.5, 1.5)
    router = normal_values(arg_keys[5], (D, EXPERTS), D ** -0.5, 0.25)
    expert_in = normal_values(arg_keys[6], (EXPERTS, D, HID), D ** -0.5, 0.25, ((0, 16), (2, 2)))
    expert_out = normal_values(arg_keys[7], (EXPERTS, HID, D), HID ** -0.5, 0.125, ((0, 16), (1, 2)))
    moe_gain = jnp.clip(1.0 + 0.1 * jax.random.normal(arg_keys[8], (D,), jnp.float32), 0.5, 1.5)
    expert_ids_keys = jax.random.split(jax.random.fold_in(arg_keys[9], 1), N_TALL * N_WIDE * TOK_DEV // TOK_DEV)
    expert_ids_turns = jax.random.permutation(jax.random.fold_in(arg_keys[9], 3), N_TALL * N_WIDE * TOK_DEV // TOK_DEV)
    expert_ids = jax.vmap(lambda own, number: shared_out(jax.random.fold_in(arg_keys[9], 2), own, number, TOK_DEV, EXPERTS, 1, CAP, 2))(expert_ids_keys, expert_ids_turns).reshape((N_TALL, N_WIDE, TOK_DEV, 1))
    keep = plant((jax.random.randint(arg_keys[10], (N_TALL, N_WIDE, TOK_DEV), 0, 8) < 7).astype(jnp.int32), jax.random.fold_in(arg_keys[10], 1), 0, 1)
    return dict(tokens=tokens, qkv_weight=qkv_weight, proj_weight=proj_weight, head_scale=head_scale, attn_gain=attn_gain, router=router, expert_in=expert_in, expert_out=expert_out, moe_gain=moe_gain, expert_ids=expert_ids, keep=keep)


def normalize(values_in, gain_vec):
    average = lax.optimization_barrier(jnp.mean(values_in, axis=-1, keepdims=True))
    centered = values_in - average
    spread = lax.optimization_barrier(jnp.mean(centered * centered, axis=-1, keepdims=True))
    return centered * lax.rsqrt(spread + 1e-05) * gain_vec

def unit_heads(block, head_count):
    shaped = block.reshape(block.shape[0], head_count, -1)
    return (shaped * lax.rsqrt(lax.optimization_barrier(jnp.sum(shaped * shaped, axis=-1, keepdims=True)) + 1e-06)).astype(jnp.bfloat16)

def window_out(window, first_row, first_col, qkv_weight, proj_weight, head_scale, attn_gain):
    window_len = WIN * WIN
    offsets = jnp.arange(window_len, dtype=jnp.int32)
    row_index = first_row + offsets // WIN
    col_index = first_col + offsets % WIN
    region = (row_index + SHIFT >= NH).astype(jnp.int32) * 2 + (col_index + SHIFT >= NW).astype(jnp.int32)
    masking = jnp.where(region[:, None] == region[None, :], 0.0, -100.0).astype(jnp.float32)
    project = jnp.dot(window, qkv_weight, preferred_element_type=jnp.float32)
    queries = unit_heads(project[:, :D], HEADS)
    key_heads = unit_heads(project[:, D:2 * D], HEADS)
    value_heads = project[:, 2 * D:].astype(jnp.bfloat16).reshape(window_len, HEADS, HEAD_DIM)
    scores = jnp.einsum('qhd,khd->hqk', queries.astype(jnp.float32), key_heads.astype(jnp.float32))
    scores = scores * head_scale[:, None, None] + masking[None]
    weights_soft = jax.nn.softmax(scores, axis=-1).astype(jnp.bfloat16)
    attended = jnp.einsum('hqk,khd->qhd', weights_soft.astype(jnp.float32), value_heads.astype(jnp.float32))
    attended = attended.astype(jnp.bfloat16).reshape(window_len, D)
    output = jnp.dot(attended, proj_weight, preferred_element_type=jnp.float32)
    return (window.astype(jnp.float32) + normalize(output, attn_gain)).astype(jnp.bfloat16)

def expert_row(tile_rows, route_ids, keep_flag, router, expert_in, expert_out, moe_gain):
    onehot = (route_ids[..., None] == jnp.arange(EXPERTS, dtype=jnp.int32)).astype(jnp.int32)
    live_hits = onehot * keep_flag[..., None]
    before = jnp.cumsum(live_hits, axis=1) - live_hits
    slot_ids = lax.optimization_barrier(jnp.sum(before * onehot, axis=-1))
    target = jnp.where(keep_flag == 1, route_ids * CAP + slot_ids, EXPERTS * CAP).astype(jnp.int32)
    sources = jnp.broadcast_to(jnp.arange(N_WIDE, dtype=jnp.int32)[:, None], target.shape)
    buffer = jnp.zeros((N_WIDE, EXPERTS * CAP + 1, D), jnp.bfloat16).at[sources, target].set(tile_rows)
    grouped = buffer[:, :EXPERTS * CAP].reshape(N_WIDE, EXPERTS, CAP, D).transpose(1, 0, 2, 3)
    grouped = grouped.reshape(EXPERTS, N_WIDE * CAP, D)
    hidden = jnp.einsum('erd,edh->erh', grouped.astype(jnp.float32), expert_in.astype(jnp.float32))
    hidden = jax.nn.gelu(hidden, approximate=False).astype(jnp.bfloat16)
    produced = jnp.einsum('erh,ehd->erd', hidden.astype(jnp.float32), expert_out.astype(jnp.float32)).astype(jnp.bfloat16)
    back = produced.reshape(EXPERTS, N_WIDE, CAP, D).transpose(1, 0, 2, 3).reshape(N_WIDE, EXPERTS * CAP, D)
    back = jnp.concatenate([back, jnp.zeros((N_WIDE, 1, D), jnp.bfloat16)], axis=1)
    picked = jnp.take_along_axis(back, target[..., None], axis=1)
    logits = jnp.einsum('wtd,de->wte', tile_rows.astype(jnp.float32), router.astype(jnp.float32))
    gate_prob = jax.nn.sigmoid(lax.optimization_barrier(jnp.sum(logits * onehot.astype(jnp.float32), axis=-1)))
    scaled = keep_flag.astype(jnp.float32) * gate_prob
    return (tile_rows.astype(jnp.float32) + scaled[..., None] * normalize(picked.astype(jnp.float32), moe_gain)).astype(jnp.bfloat16)

def reference(tokens, qkv_weight, proj_weight, head_scale, attn_gain, router, expert_in, expert_out, moe_gain, expert_ids, keep):
    rolled = jnp.roll(tokens, (-SHIFT, -SHIFT), axis=(0, 1))
    across = NW // WIN
    windows = rolled.reshape(NH // WIN, WIN, across, WIN, D).transpose(0, 2, 1, 3, 4).reshape(-1, WIN * WIN, D)
    numbers = jnp.arange(windows.shape[0], dtype=jnp.int32)
    first_rows = numbers // across * WIN
    first_cols = numbers % across * WIN
    mixed_in = lax.map(lambda pieces: window_out(pieces[0], pieces[1], pieces[2], qkv_weight, proj_weight, head_scale, attn_gain), (windows, first_rows, first_cols))
    grid = mixed_in.reshape(NH // WIN, across, WIN, WIN, D).transpose(0, 2, 1, 3, 4).reshape(NH, NW, D)
    tiles = grid.reshape(N_TALL, TILE_H, N_WIDE, WIN, D).transpose(0, 2, 1, 3, 4).reshape(N_TALL, N_WIDE, TOK_DEV, D)
    rows_out = lax.map(lambda pieces: expert_row(pieces[0], pieces[1], pieces[2], router, expert_in, expert_out, moe_gain), (tiles, expert_ids[..., 0], keep))
    return rows_out.reshape(N_TALL, N_WIDE, TILE_H, WIN, D).transpose(0, 2, 1, 3, 4).reshape(NH, NW, D)
```

```python
import functools

import jax
import jax.numpy as jnp
from jax import lax
from jax.experimental import pallas as pl
from jax.experimental.pallas import tpu as pltpu
from jax.sharding import PartitionSpec as P

LANES = 128
LOG2E = 1.4426950408889634
VMEM_LIMIT = 48 * 1024 * 1024


def shifted(value, axis, by):
    peers = lax.axis_size(axis)
    return lax.ppermute(value, axis, [(i, (i + by) % peers) for i in range(peers)])


def dot(a, b):
    return jnp.dot(a, b, preferred_element_type=jnp.float32)


def dot_nt(a, b):
    return lax.dot_general(a, b, (((1,), (1,)), ((), ())), preferred_element_type=jnp.float32)


def attn_kernel(
    grid_rc,
    head_dim,
    edge,
    rows_q,
    first_ref,
    scale_ref,
    win_ref,
    wqkv_ref,
    wproj_ref,
    gain_ref,
    target_ref,
    x1_ref,
    sent_ref,
    qn_s,
    kcat_s,
    vcat_s,
    att_s,
):
    total_rows, total_cols, shift = grid_rc
    count, feature = win_ref.shape
    groups = feature // LANES
    per_group = LANES // head_dim
    win = win_ref[...]

    flat = lax.broadcasted_iota(jnp.int32, (count, LANES), 0)
    lane = lax.broadcasted_iota(jnp.int32, (count, LANES), 1)
    low = (first_ref[0] + flat // edge + shift >= total_rows).astype(jnp.int32)
    right = (first_ref[1] + flat % edge + shift >= total_cols).astype(jnp.int32)
    region = 2 * low + right
    same = region == lane // 3
    kfeat = jnp.where((lane < 12) & jnp.logical_not(same), 1.0, 0.0).astype(jnp.bfloat16)
    ones = jnp.ones((count, LANES), jnp.bfloat16)
    for g in range(groups):
        kcat_s[g, :, LANES:] = kfeat
        vcat_s[g, :, LANES:] = ones

    wide = 2 * LANES
    r_i = lax.broadcasted_iota(jnp.int32, (wide, wide), 0) // head_dim
    c_i = lax.broadcasted_iota(jnp.int32, (wide, wide), 1) // head_dim
    block = jnp.where(r_i == c_i, 1.0, 0.0).astype(jnp.bfloat16)

    def unit(value):
        sq = value * value
        hi = sq.astype(jnp.bfloat16)
        lo = (sq - hi.astype(jnp.float32)).astype(jnp.bfloat16)
        total = dot(hi, block) + dot(lo, block)
        return (value * lax.rsqrt(total + 1e-06)).astype(jnp.bfloat16)

    for p in range(feature // wide):
        at = p * wide
        qn_s[:, at : at + wide] = unit(dot(win, wqkv_ref[:, at : at + wide]))
        kn = unit(dot(win, wqkv_ref[:, feature + at : feature + at + wide]))
        vb = dot(win, wqkv_ref[:, 2 * feature + at : 2 * feature + at + wide]).astype(jnp.bfloat16)
        for half in range(2):
            kcat_s[2 * p + half, :, :LANES] = kn[:, half * LANES : (half + 1) * LANES]
            vcat_s[2 * p + half, :, :LANES] = vb[:, half * LANES : (half + 1) * LANES]

    blocks = count // rows_q
    lane_q = lax.broadcasted_iota(jnp.int32, (rows_q, LANES), 1)
    lane_head = lane_q // head_dim
    part = lane_q % 3

    def step(index, carry):
        g = index // blocks
        row = pl.multiple_of((index % blocks) * rows_q, rows_q)
        col = pl.multiple_of(g * LANES, LANES)
        q = qn_s[pl.ds(row, rows_q), pl.ds(col, LANES)]
        kcat = kcat_s[g]
        vcat = vcat_s[g]
        flat_q = row + lax.broadcasted_iota(jnp.int32, (rows_q, LANES), 0)
        low_q = (first_ref[0] + flat_q // edge + shift >= total_rows).astype(jnp.int32)
        right_q = (first_ref[1] + flat_q % edge + shift >= total_cols).astype(jnp.int32)
        same_q = (2 * low_q + right_q == lane_q // 3) & (lane_q < 12)
        num = jnp.zeros((rows_q, LANES), jnp.float32)
        den = jnp.ones((rows_q, LANES), jnp.float32)
        for h in range(per_group):
            scale = scale_ref[g * per_group + h]
            off = jnp.full((rows_q, LANES), -100.0, jnp.float32) / scale
            b0 = off.astype(jnp.bfloat16).astype(jnp.float32)
            b1 = (off - b0).astype(jnp.bfloat16).astype(jnp.float32)
            b2 = off - b0 - b1
            piece = jnp.where(part == 0, b0, jnp.where(part == 1, b1, b2))
            qfeat = jnp.where(same_q, piece, 0.0).astype(jnp.bfloat16)
            qh = jnp.where(lane_head == h, q, jnp.zeros_like(q))
            s = dot_nt(jnp.concatenate([qh, qfeat], axis=1), kcat)
            top = jnp.max(s, axis=1, keepdims=True)
            e = jnp.exp2((s - top) * (scale * LOG2E)).astype(jnp.bfloat16)
            o = dot(e, vcat)
            num = jnp.where(lane_head == h, o[:, :LANES], num)
            den = jnp.where(lane_head == h, o[:, LANES:], den)
        att_s[pl.ds(row, rows_q), pl.ds(col, LANES)] = (num / den).astype(jnp.bfloat16)
        return carry

    lax.fori_loop(0, groups * blocks, step, 0)

    out = dot(att_s[...], wproj_ref[...])
    mean = jnp.mean(out, axis=1, keepdims=True)
    cent = out - mean
    var = jnp.mean(cent * cent, axis=1, keepdims=True)
    x1 = (win.astype(jnp.float32) + cent * lax.rsqrt(var + 1e-05) * gain_ref[...]).astype(jnp.bfloat16)
    x1_ref[...] = x1

    target = target_ref[...]
    slots = sent_ref.shape[0]
    chunk = slots // 4
    for i in range(4):
        slot = i * chunk + lax.broadcasted_iota(jnp.int32, (chunk, count), 0)
        pick = jnp.where(slot == target, 1.0, 0.0).astype(jnp.bfloat16)
        sent_ref[i * chunk : (i + 1) * chunk, :] = dot(pick, x1).astype(jnp.bfloat16)


def expert_kernel(parts, row_block, x_ref, *refs):
    w_in, w_out, y_ref = refs[:parts], refs[parts : 2 * parts], refs[2 * parts]
    rows = x_ref.shape[0]

    def step(i, carry):
        row = pl.multiple_of(i * row_block, row_block)
        x = x_ref[pl.ds(row, row_block), :]
        total = None
        for n in range(parts):
            h = dot(x, w_in[n][...])
            h = (0.5 * h * (1.0 + lax.erf(h * 0.7071067811865476))).astype(jnp.bfloat16)
            y = dot(h, w_out[n][...])
            total = y if total is None else total + y
        y_ref[pl.ds(row, row_block), :] = total.astype(jnp.bfloat16)
        return carry

    lax.fori_loop(0, rows // row_block, step, 0)


def combine_kernel(row_block, back_ref, x1_ref, target_ref, scaled_ref, gain_ref, out_ref):
    count = x1_ref.shape[0]
    slots = back_ref.shape[0]

    def step(i, carry):
        row = pl.multiple_of(i * row_block, row_block)
        at = pl.ds(row, row_block)
        slot = lax.broadcasted_iota(jnp.int32, (row_block, slots), 1)
        pick = jnp.where(slot == target_ref[at, :], 1.0, 0.0).astype(jnp.bfloat16)
        y = dot(pick, back_ref[...])
        mean = jnp.mean(y, axis=1, keepdims=True)
        cent = y - mean
        var = jnp.mean(cent * cent, axis=1, keepdims=True)
        add = scaled_ref[at, :] * (cent * lax.rsqrt(var + 1e-05) * gain_ref[...])
        out_ref[at, :] = (x1_ref[at, :].astype(jnp.float32) + add).astype(jnp.bfloat16)
        return carry

    lax.fori_loop(0, count // row_block, step, 0)


def params():
    return pltpu.CompilerParams(vmem_limit_bytes=VMEM_LIMIT)


VM = pl.BlockSpec(memory_space=pltpu.VMEM)
SM = pl.BlockSpec(memory_space=pltpu.SMEM)


def body(
    tokens,
    qkv_weight,
    proj_weight,
    head_scale,
    attn_gain,
    router,
    expert_in,
    expert_out,
    moe_gain,
    expert_ids,
    keep,
):
    tile_rows, edge, feature = tokens.shape
    shift = edge // 2
    tall = lax.axis_size("tall")
    count = tile_rows * edge

    column_part = shifted(tokens[:, :shift], "wide", -1)
    widened = jnp.concatenate([tokens[:, shift:], column_part], axis=1)
    row_part = shifted(widened[:shift], "tall", -1)
    rolled = jnp.concatenate([widened[shift:], row_part], axis=0).reshape(count, feature)

    w_in = [expert_in[0]] + [shifted(expert_in[0], "tall", -n) for n in range(1, tall)]
    w_out = [expert_out[0]] + [shifted(expert_out[0], "tall", -n) for n in range(1, tall)]

    total_rows = tile_rows * tall
    total_cols = edge * lax.axis_size("wide")
    first = jnp.stack([lax.axis_index("tall") * tile_rows, lax.axis_index("wide") * edge]).astype(jnp.int32)

    route_ids = expert_ids[0, 0, :, 0]
    keep_flag = keep[0, 0]
    experts = router.shape[1]
    capacity = max(2, 3 * count // (2 * experts))
    room = -(-capacity // 8) * 8
    onehot = (route_ids[:, None] == jnp.arange(experts, dtype=jnp.int32)[None, :]).astype(jnp.int32)
    live_hits = onehot * keep_flag[:, None]
    before = jnp.cumsum(live_hits, axis=0) - live_hits
    slot_ids = jnp.sum(before * onehot, axis=1)
    target = jnp.where(keep_flag == 1, route_ids * room + slot_ids, experts * room)

    head_dim = feature // head_scale.shape[0]
    slots = experts * room
    groups = feature // LANES
    x1, sent = pl.pallas_call(
        functools.partial(attn_kernel, (total_rows, total_cols, shift), head_dim, edge, count // 3),
        out_shape=(
            jax.ShapeDtypeStruct((count, feature), jnp.bfloat16),
            jax.ShapeDtypeStruct((slots, feature), jnp.bfloat16),
        ),
        in_specs=[SM, SM, VM, VM, VM, VM, VM],
        out_specs=(VM, VM),
        scratch_shapes=[
            pltpu.VMEM((count, feature), jnp.bfloat16),
            pltpu.VMEM((groups, count, 2 * LANES), jnp.bfloat16),
            pltpu.VMEM((groups, count, 2 * LANES), jnp.bfloat16),
            pltpu.VMEM((count, feature), jnp.bfloat16),
        ],
        compiler_params=params(),
        name="attention",
    )(first, head_scale, rolled, qkv_weight, proj_weight, attn_gain[None, :], target[None, :])

    arrived = lax.all_to_all(
        sent.reshape(experts, room, feature), "wide", split_axis=0, concat_axis=0, tiled=True
    ).reshape(slots, feature)

    produced = pl.pallas_call(
        functools.partial(expert_kernel, tall, slots // 4),
        out_shape=jax.ShapeDtypeStruct((slots, feature), jnp.bfloat16),
        in_specs=[VM] * (1 + 2 * tall),
        out_specs=VM,
        compiler_params=params(),
        name="experts",
    )(arrived, *w_in, *w_out)

    returned = lax.all_to_all(
        produced.reshape(experts, room, feature), "wide", split_axis=0, concat_axis=0, tiled=True
    ).reshape(slots, feature)

    logits = dot(x1, router)
    gate_prob = jax.nn.sigmoid(jnp.sum(logits * onehot.astype(jnp.float32), axis=1))
    scaled = keep_flag.astype(jnp.float32) * gate_prob
    result = pl.pallas_call(
        functools.partial(combine_kernel, count // 4),
        out_shape=jax.ShapeDtypeStruct((count, feature), jnp.bfloat16),
        in_specs=[VM] * 5,
        out_specs=VM,
        compiler_params=params(),
        name="combine",
    )(returned, x1, target[:, None], scaled[:, None], moe_gain[None, :])
    return result.reshape(tile_rows, edge, feature)


def solution(mesh):
    placed = (
        P("tall", "wide", None),
        P(),
        P(),
        P(),
        P(),
        P(),
        P("wide", None, "tall"),
        P("wide", "tall", None),
        P(),
        P("tall", "wide", None, None),
        P("tall", "wide", None),
    )
    return jax.shard_map(
        body, mesh=mesh, in_specs=placed, out_specs=P("tall", "wide", None), check_vma=False
    )
```

```python
import functools

import jax
import jax.numpy as jnp
from jax import lax
from jax.experimental import pallas as pl
from jax.experimental.pallas import tpu as pltpu
from jax.sharding import PartitionSpec as P

LANES = 128
VM = pl.BlockSpec(memory_space=pltpu.VMEM)
SM = pl.BlockSpec(memory_space=pltpu.SMEM)
HB = pl.BlockSpec(memory_space=pltpu.HBM)
LOG2E = 1.4426950408889634


CHUNKS = 1


def chunk_sizes(room):
    tiles = room // 8
    count = min(CHUNKS, tiles)
    return [8 * (tiles * (i + 1) // count - tiles * i // count) for i in range(count)]


def shifted(value, axis, by):
    peers = lax.axis_size(axis)
    return lax.ppermute(value, axis, [(i, (i + by) % peers) for i in range(peers)])


def dot(a, b):
    return jnp.dot(a, b, preferred_element_type=jnp.float32)


def attn_kernel(
    grid_rc,
    head_dim,
    edge,
    rows_q,
    stop,
    unroll,
    first_ref,
    scale_ref,
    win_ref,
    wqkv_ref,
    wproj_ref,
    gain_ref,
    target_ref,
    x1_ref,
    *rest_refs,
):
    *sent_refs, q_s, att_s, kbig_s, vbig_s, sa_s, sb_s, out_s, sem = rest_refs
    total_rows, total_cols, shift = grid_rc
    count, feature = win_ref.shape
    groups = feature // LANES
    heads = LANES // head_dim
    main = count // LANES * LANES
    rest = count - main
    regions, terms = 4, 3
    feats = regions * terms
    win = win_ref[...]

    flat = lax.broadcasted_iota(jnp.int32, (count, LANES), 0)
    lane = lax.broadcasted_iota(jnp.int32, (count, LANES), 1)
    low = (first_ref[0] + flat // edge + shift >= total_rows).astype(jnp.int32)
    right = (first_ref[1] + flat % edge + shift >= total_cols).astype(jnp.int32)
    used = lane < heads * feats
    same = (2 * low + right) == (lane % feats) // terms
    kfeat = jnp.where(used & jnp.logical_not(same), 1.0, 0.0).astype(jnp.bfloat16)
    qmatch = used & same

    wide = 2 * LANES
    r_i = lax.broadcasted_iota(jnp.int32, (wide, wide), 0) // head_dim
    c_i = lax.broadcasted_iota(jnp.int32, (wide, wide), 1) // head_dim
    block = jnp.where(r_i == c_i, 1.0, 0.0).astype(jnp.bfloat16)

    def unit(value):
        sq = value * value
        hi = sq.astype(jnp.bfloat16)
        lo = (sq - hi.astype(jnp.float32)).astype(jnp.bfloat16)
        total = dot(hi, block) + dot(lo, block)
        return (value * lax.rsqrt(total + 1e-06)).astype(jnp.bfloat16)

    head_of = lane // head_dim
    krow = lax.broadcasted_iota(jnp.int32, (wide, LANES), 0)
    khead = jnp.where(krow < LANES, krow // head_dim, (krow - LANES) // feats)
    klane = lax.broadcasted_iota(jnp.int32, (wide, LANES), 1)
    lane1 = lax.broadcasted_iota(jnp.int32, (8, LANES), 1)
    lane_head = lane1 // feats
    lane_term = lane1 % terms
    zero = jnp.zeros((), jnp.bfloat16)
    per_tile = LANES // rest if rest else 1
    kfeat_t = kfeat.T
    ones = [jnp.where(head_of == h, 1.0, 0.0).astype(jnp.bfloat16) for h in range(heads)]

    def place(g, q, k, v):
        kt = jnp.concatenate([k.T, kfeat_t], axis=0)
        for h in range(heads):
            for t in range(main // LANES):
                kbig_s[g, :, h * main + t * LANES : h * main + (t + 1) * LANES] = jnp.where(
                    khead == h, kt[:, t * LANES : (t + 1) * LANES], zero
                )
            vm = jnp.concatenate([jnp.where(head_of == h, v, zero), ones[h]], axis=1)
            vbig_s[g, h * main : (h + 1) * main, :] = vm[:main]
            if rest:
                vbig_s[g, heads * main + h * rest : heads * main + (h + 1) * rest, :] = vm[main:]
        if rest:
            tail = jnp.concatenate([kt[:, main:]] * per_tile, axis=1)
            for t in range(heads // per_tile):
                kbig_s[g, :, heads * main + t * LANES : heads * main + (t + 1) * LANES] = jnp.where(
                    khead == t * per_tile + klane // rest, tail, zero
                )
        scale = jnp.full((8, LANES), scale_ref[g * heads], jnp.float32)
        for h in range(1, heads):
            scale = jnp.where(lane_head == h, scale_ref[g * heads + h], scale)
        off = -100.0 / scale
        b0 = off.astype(jnp.bfloat16).astype(jnp.float32)
        b1 = (off - b0).astype(jnp.bfloat16).astype(jnp.float32)
        b2 = off - b0 - b1
        piece = jnp.where(lane_term == 0, b0, jnp.where(lane_term == 1, b1, b2))[:1]
        q_s[g, :, :LANES] = q
        q_s[g, :, LANES:] = jnp.where(qmatch, piece, 0.0).astype(jnp.bfloat16)

    for p in range(feature // wide):
        at = p * wide
        qn = unit(dot(win, wqkv_ref[:, at : at + wide]))
        kn = unit(dot(win, wqkv_ref[:, feature + at : feature + at + wide]))
        vb = dot(win, wqkv_ref[:, 2 * feature + at : 2 * feature + at + wide]).astype(jnp.bfloat16)
        for half in range(2):
            part = slice(half * LANES, (half + 1) * LANES)
            place(2 * p + half, qn[:, part], kn[:, part], vb[:, part])
    if stop < 1:
        x1_ref[...] = win
        return

    tail_lane = lax.broadcasted_iota(jnp.int32, (rows_q, LANES), 1)

    def scores(g, b):
        return dot(q_s[g, pl.ds(b * rows_q, rows_q), :], kbig_s[g])

    def finish(g, b, s_ref):
        factors = [scale_ref[g * heads + h] * LOG2E for h in range(heads)]
        tops, es = [], []
        for h in range(heads):
            tiles = [s_ref[:, h * main + t * LANES : h * main + (t + 1) * LANES] for t in range(main // LANES)]
            if rest:
                t = h // per_tile
                tile = s_ref[:, heads * main + t * LANES : heads * main + (t + 1) * LANES]
                tiles.append(jnp.where(tail_lane // rest == h % per_tile, tile, -3e38))
            top = functools.reduce(jnp.maximum, tiles)
            tops.append(jnp.max(top, axis=1, keepdims=True))
        for h in range(heads):
            e = jnp.exp2((s_ref[:, h * main : (h + 1) * main] - tops[h]) * factors[h])
            es.append(e.astype(jnp.bfloat16))
        if rest:
            for t in range(heads // per_tile):
                top = jnp.broadcast_to(tops[t * per_tile], (rows_q, LANES))
                factor = jnp.full((rows_q, LANES), factors[t * per_tile], jnp.float32)
                for j in range(1, per_tile):
                    top = jnp.where(tail_lane // rest == j, tops[t * per_tile + j], top)
                    factor = jnp.where(tail_lane // rest == j, factors[t * per_tile + j], factor)
                tile = s_ref[:, heads * main + t * LANES : heads * main + (t + 1) * LANES]
                es.append(jnp.exp2((tile - top) * factor).astype(jnp.bfloat16))
        o = dot(jnp.concatenate(es, axis=1), vbig_s[g])
        col = g * LANES if isinstance(g, int) else pl.multiple_of(g * LANES, LANES)
        att_s[b * rows_q : (b + 1) * rows_q, pl.ds(col, LANES)] = (o[:, :LANES] / o[:, LANES:]).astype(jnp.bfloat16)

    blocks = count // rows_q
    bufs = [sa_s, sb_s]
    sa_s[...] = scores(0, 0)
    if unroll:
        work = [(g, b) for g in range(groups) for b in range(blocks)]
        for i, (g, b) in enumerate(work):
            if i + 1 < len(work):
                bufs[(i + 1) % 2][...] = scores(*work[i + 1])
            finish(g, b, bufs[i % 2])
    else:
        def step(g, carry):
            for b in range(blocks):
                nxt = (g, b + 1) if b + 1 < blocks else (jnp.minimum(g + 1, groups - 1), 0)
                bufs[(b + 1) % 2][...] = scores(*nxt)
                finish(g, b, bufs[b % 2])
            return carry

        lax.fori_loop(0, groups, step, 0)
    if stop < 2:
        x1_ref[...] = att_s[...]
        return

    out = dot(att_s[...], wproj_ref[...])
    mean = jnp.mean(out, axis=1, keepdims=True)
    cent = out - mean
    var = jnp.mean(cent * cent, axis=1, keepdims=True)
    x1 = (win.astype(jnp.float32) + cent * lax.rsqrt(var + 1e-05) * gain_ref[...]).astype(jnp.bfloat16)
    x1_ref[...] = x1

    if stop < 3:
        return
    target = target_ref[...]
    copies, base = [], 0
    for i, sent_ref in enumerate(sent_refs):
        rows = sent_ref.shape[0]
        slot = base + lax.broadcasted_iota(jnp.int32, (rows, count), 0)
        pick = jnp.where(slot == target, 1.0, 0.0).astype(jnp.bfloat16)
        out_s[base : base + rows, :] = dot(pick, x1).astype(jnp.bfloat16)
        copies.append(pltpu.make_async_copy(out_s.at[pl.ds(base, rows)], sent_ref, sem.at[i]))
        copies[-1].start()
        base += rows
    for copy in copies:
        copy.wait()


def call_attn(first, head_scale, rolled, qkv, proj, gain, target, *, grid_rc, edge, sizes, rows_q=None, stop=9, unroll=1):
    count, feature = rolled.shape
    rows_q = rows_q or count // 2
    head_dim = feature // head_scale.shape[0]
    groups = feature // LANES
    return pl.pallas_call(
        functools.partial(attn_kernel, grid_rc, head_dim, edge, rows_q, stop, unroll),
        out_shape=(
            jax.ShapeDtypeStruct((count, feature), jnp.bfloat16),
            *[pltpu.HBM((rows, feature), jnp.bfloat16) for rows in sizes],
        ),
        in_specs=[SM, SM, VM, VM, VM, VM, VM],
        out_specs=(VM, *[HB] * len(sizes)),
        scratch_shapes=[
            pltpu.VMEM((groups, count, 2 * LANES), jnp.bfloat16),
            pltpu.VMEM((count, feature), jnp.bfloat16),
            pltpu.VMEM((groups, 2 * LANES, LANES // head_dim * count), jnp.bfloat16),
            pltpu.VMEM((groups, LANES // head_dim * count, 2 * LANES), jnp.bfloat16),
            pltpu.VMEM((rows_q, LANES // head_dim * count), jnp.float32),
            pltpu.VMEM((rows_q, LANES // head_dim * count), jnp.float32),
            pltpu.VMEM((sum(sizes), feature), jnp.bfloat16),
            pltpu.SemaphoreType.DMA((len(sizes),)),
        ],
        compiler_params=pltpu.CompilerParams(vmem_limit_bytes=32 * 1024 * 1024),
        name="attention",
    )(first, head_scale, rolled, qkv, proj, gain, target)


def expert_kernel(parts, row_block, x_ref, *refs):
    w_in, w_out, y_ref = refs[:parts], refs[parts : 2 * parts], refs[2 * parts]
    in_s, out_s, acc_s, sem = refs[2 * parts + 1 :]
    rows = x_ref.shape[0]
    copies = []
    for n in range(parts):
        copies.append(pltpu.make_async_copy(w_in[n], in_s.at[n], sem.at[2 * n]))
        copies.append(pltpu.make_async_copy(w_out[n], out_s.at[n], sem.at[2 * n + 1]))
    for copy in copies:
        copy.start()
    for n in range(parts):
        copies[2 * n].wait()
        copies[2 * n + 1].wait()
        for i in range(rows // row_block):
            part = slice(i * row_block, (i + 1) * row_block)
            h = dot(x_ref[part, :], in_s[n])
            h = (0.5 * h * (1.0 + lax.erf(h * 0.7071067811865476))).astype(jnp.bfloat16)
            y = dot(h, out_s[n])
            if n:
                y = acc_s[part, :] + y
            if n < parts - 1:
                acc_s[part, :] = y
            else:
                y_ref[part, :] = y.astype(jnp.bfloat16)


def gate_kernel(x1_ref, router_ref, target_ref, ids_ref, pick_ref, scaled_ref):
    count, slots = pick_ref.shape
    target = target_ref[...]
    slot = lax.broadcasted_iota(jnp.int32, (count, slots), 1)
    pick_ref[...] = jnp.where(slot == target, 1.0, 0.0).astype(jnp.bfloat16)
    logits = dot(x1_ref[...], router_ref[...])
    mine = lax.broadcasted_iota(jnp.int32, logits.shape, 1) == ids_ref[...]
    logit = jnp.sum(jnp.where(mine, logits, 0.0), axis=1, keepdims=True)
    scaled_ref[...] = jnp.where(target < slots, jax.nn.sigmoid(logit), 0.0)


def combine_kernel(row_block, x1_ref, pick_ref, scaled_ref, gain_ref, *refs):
    *back_refs, out_ref = refs
    for i in range(x1_ref.shape[0] // row_block):
        at = slice(i * row_block, (i + 1) * row_block)
        y, base = None, 0
        for back_ref in back_refs:
            rows = back_ref.shape[0]
            term = dot(pick_ref[at, base : base + rows], back_ref[...])
            y = term if y is None else y + term
            base += rows
        mean = jnp.mean(y, axis=1, keepdims=True)
        cent = y - mean
        var = jnp.mean(cent * cent, axis=1, keepdims=True)
        add = scaled_ref[at, :] * (cent * lax.rsqrt(var + 1e-05) * gain_ref[...])
        out_ref[at, :] = (x1_ref[at, :].astype(jnp.float32) + add).astype(jnp.bfloat16)


def params(mib):
    return pltpu.CompilerParams(vmem_limit_bytes=mib * 1024 * 1024)


def body(
    tokens,
    qkv_weight,
    proj_weight,
    head_scale,
    attn_gain,
    router,
    expert_in,
    expert_out,
    moe_gain,
    expert_ids,
    keep,
):
    tile_rows, edge, feature = tokens.shape
    shift = edge // 2
    tall = lax.axis_size("tall")
    count = tile_rows * edge

    column_part = shifted(tokens[:, :shift], "wide", -1)
    widened = jnp.concatenate([tokens[:, shift:], column_part], axis=1)
    row_part = shifted(widened[:shift], "tall", -1)
    rolled = jnp.concatenate([widened[shift:], row_part], axis=0).reshape(count, feature)

    w_in = [expert_in[0]] + [shifted(expert_in[0], "tall", -n) for n in range(1, tall)]
    w_out = [expert_out[0]] + [shifted(expert_out[0], "tall", -n) for n in range(1, tall)]

    total_rows = tile_rows * tall
    total_cols = edge * lax.axis_size("wide")
    first = jnp.stack([lax.axis_index("tall") * tile_rows, lax.axis_index("wide") * edge]).astype(jnp.int32)

    route_ids = expert_ids[0, 0, :, 0]
    keep_flag = keep[0, 0]
    experts = router.shape[1]
    capacity = max(2, 3 * count // (2 * experts))
    room = -(-capacity // 8) * 8
    onehot = (route_ids[:, None] == jnp.arange(experts, dtype=jnp.int32)[None, :]).astype(jnp.int32)
    live_hits = onehot * keep_flag[:, None]
    before = jnp.cumsum(live_hits, axis=0) - live_hits
    slot_ids = jnp.sum(before * onehot, axis=1)
    parts = chunk_sizes(room)
    slots = experts * room
    row, start = jnp.zeros_like(slot_ids), 0
    for part in parts:
        here = experts * start + route_ids * part + slot_ids - start
        row = jnp.where((slot_ids >= start) & (slot_ids < start + part), here, row)
        start += part
    target = jnp.where(keep_flag == 1, row, slots)

    x1, *sent = call_attn(
        first,
        head_scale,
        rolled,
        qkv_weight,
        proj_weight,
        attn_gain[None, :],
        target[None, :],
        grid_rc=(total_rows, total_cols, shift),
        edge=edge,
        sizes=tuple(experts * part for part in parts),
    )
    hidden = w_in[0].shape[1]
    weights = [pltpu.with_memory_space_constraint(w, pltpu.HBM) for w in w_in + w_out]

    def exchange(value):
        rows = value.shape[0]
        value = value.reshape(experts, rows // experts, feature)
        return lax.all_to_all(value, "wide", split_axis=0, concat_axis=0, tiled=True).reshape(rows, feature)

    def run_experts(value):
        rows = value.shape[0]
        return pl.pallas_call(
            functools.partial(expert_kernel, tall, rows // 2 if rows > 512 else rows),
            out_shape=pltpu.HBM((rows, feature), jnp.bfloat16),
            in_specs=[VM] + [HB] * (2 * tall),
            out_specs=VM,
            scratch_shapes=[
                pltpu.VMEM((tall, feature, hidden), jnp.bfloat16),
                pltpu.VMEM((tall, hidden, feature), jnp.bfloat16),
                pltpu.VMEM((rows, feature), jnp.float32),
                pltpu.SemaphoreType.DMA((2 * tall,)),
            ],
            compiler_params=params(32),
            cost_estimate=pl.CostEstimate(
                flops=4 * rows * feature * hidden * tall, bytes_accessed=4 * feature * hidden * tall, transcendentals=0
            ),
        )(value, *weights)

    arrived = []
    for value in sent:
        arrived.append(exchange(value))
    returned = []
    for value in arrived:
        made = run_experts(value)
        returned.append(exchange(made))

    pick, scaled = pl.pallas_call(
        gate_kernel,
        out_shape=(
            jax.ShapeDtypeStruct((count, slots), jnp.bfloat16),
            jax.ShapeDtypeStruct((count, 1), jnp.float32),
        ),
        in_specs=[VM] * 4,
        out_specs=(VM, VM),
        compiler_params=params(16),
        name="gate",
    )(x1, router, target[:, None], route_ids[:, None])
    result = pl.pallas_call(
        functools.partial(combine_kernel, count // 2),
        out_shape=jax.ShapeDtypeStruct((count, feature), jnp.bfloat16),
        in_specs=[VM] * (4 + len(parts)),
        out_specs=VM,
        compiler_params=params(16),
        name="combine",
    )(x1, pick, scaled, moe_gain[None, :], *returned)
    return result.reshape(tile_rows, edge, feature)


def solution(mesh):
    placed = (
        P("tall", "wide", None),
        P(),
        P(),
        P(),
        P(),
        P(),
        P("wide", None, "tall"),
        P("wide", "tall", None),
        P(),
        P("tall", "wide", None, None),
        P("tall", "wide", None),
    )
    return jax.shard_map(
        body, mesh=mesh, in_specs=placed, out_specs=P("tall", "wide", None), check_vma=False
    )
```

```python
import functools

import jax
import jax.numpy as jnp
from jax import lax
from jax.experimental import pallas as pl
from jax.experimental.pallas import tpu as pltpu
from jax.sharding import PartitionSpec as P

LANES = 128
VM = pl.BlockSpec(memory_space=pltpu.VMEM)
SM = pl.BlockSpec(memory_space=pltpu.SMEM)
HB = pl.BlockSpec(memory_space=pltpu.HBM)
LOG2E = 1.4426950408889634


CHUNKS = 1


def chunk_sizes(room):
    tiles = room // 8
    count = min(CHUNKS, tiles)
    return [8 * (tiles * (i + 1) // count - tiles * i // count) for i in range(count)]


def shifted(value, axis, by):
    peers = lax.axis_size(axis)
    return lax.ppermute(value, axis, [(i, (i + by) % peers) for i in range(peers)])


def dot(a, b):
    return jnp.dot(a, b, preferred_element_type=jnp.float32)


def attn_kernel(
    grid_rc,
    head_dim,
    edge,
    rows_q,
    stop,
    unroll,
    first_ref,
    scale_ref,
    win_ref,
    wqkv_ref,
    wproj_ref,
    gain_ref,
    target_ref,
    x1_ref,
    *rest_refs,
):
    *sent_refs, q_s, att_s, kbig_s, vbig_s, sa_s, sb_s, out_s, sem = rest_refs
    total_rows, total_cols, shift = grid_rc
    count, feature = win_ref.shape
    groups = feature // LANES
    heads = LANES // head_dim
    main = count // LANES * LANES
    rest = count - main
    regions, terms = 4, 3
    feats = regions * terms
    win = win_ref[...]

    flat = lax.broadcasted_iota(jnp.int32, (count, LANES), 0)
    lane = lax.broadcasted_iota(jnp.int32, (count, LANES), 1)
    low = (first_ref[0] + flat // edge + shift >= total_rows).astype(jnp.int32)
    right = (first_ref[1] + flat % edge + shift >= total_cols).astype(jnp.int32)
    used = lane < heads * feats
    same = (2 * low + right) == (lane % feats) // terms
    kfeat = jnp.where(used & jnp.logical_not(same), 1.0, 0.0).astype(jnp.bfloat16)
    qmatch = used & same

    wide = 2 * LANES
    r_i = lax.broadcasted_iota(jnp.int32, (wide, wide), 0) // head_dim
    c_i = lax.broadcasted_iota(jnp.int32, (wide, wide), 1) // head_dim
    block = jnp.where(r_i == c_i, 1.0, 0.0).astype(jnp.bfloat16)

    def unit(value):
        sq = value * value
        hi = sq.astype(jnp.bfloat16)
        lo = (sq - hi.astype(jnp.float32)).astype(jnp.bfloat16)
        total = dot(hi, block) + dot(lo, block)
        return (value * lax.rsqrt(total + 1e-06)).astype(jnp.bfloat16)

    head_of = lane // head_dim
    krow = lax.broadcasted_iota(jnp.int32, (wide, LANES), 0)
    khead = jnp.where(krow < LANES, krow // head_dim, (krow - LANES) // feats)
    klane = lax.broadcasted_iota(jnp.int32, (wide, LANES), 1)
    lane1 = lax.broadcasted_iota(jnp.int32, (8, LANES), 1)
    lane_head = lane1 // feats
    lane_term = lane1 % terms
    zero = jnp.zeros((), jnp.bfloat16)
    per_tile = LANES // rest if rest else 1
    kfeat_t = kfeat.T
    ones = [jnp.where(head_of == h, 1.0, 0.0).astype(jnp.bfloat16) for h in range(heads)]

    def place(g, q, k, v):
        kt = jnp.concatenate([k.T, kfeat_t], axis=0)
        for h in range(heads):
            for t in range(main // LANES):
                kbig_s[g, :, h * main + t * LANES : h * main + (t + 1) * LANES] = jnp.where(
                    khead == h, kt[:, t * LANES : (t + 1) * LANES], zero
                )
            vm = jnp.concatenate([jnp.where(head_of == h, v, zero), ones[h]], axis=1)
            vbig_s[g, h * main : (h + 1) * main, :] = vm[:main]
            if rest:
                vbig_s[g, heads * main + h * rest : heads * main + (h + 1) * rest, :] = vm[main:]
        if rest:
            tail = jnp.concatenate([kt[:, main:]] * per_tile, axis=1)
            for t in range(heads // per_tile):
                kbig_s[g, :, heads * main + t * LANES : heads * main + (t + 1) * LANES] = jnp.where(
                    khead == t * per_tile + klane // rest, tail, zero
                )
        scale = jnp.full((8, LANES), scale_ref[g * heads], jnp.float32)
        for h in range(1, heads):
            scale = jnp.where(lane_head == h, scale_ref[g * heads + h], scale)
        off = -100.0 / scale
        b0 = off.astype(jnp.bfloat16).astype(jnp.float32)
        b1 = (off - b0).astype(jnp.bfloat16).astype(jnp.float32)
        b2 = off - b0 - b1
        piece = jnp.where(lane_term == 0, b0, jnp.where(lane_term == 1, b1, b2))[:1]
        q_s[g, :, :LANES] = q
        q_s[g, :, LANES:] = jnp.where(qmatch, piece, 0.0).astype(jnp.bfloat16)

    for p in range(feature // wide):
        at = p * wide
        qn = unit(dot(win, wqkv_ref[:, at : at + wide]))
        kn = unit(dot(win, wqkv_ref[:, feature + at : feature + at + wide]))
        vb = dot(win, wqkv_ref[:, 2 * feature + at : 2 * feature + at + wide]).astype(jnp.bfloat16)
        for half in range(2):
            part = slice(half * LANES, (half + 1) * LANES)
            place(2 * p + half, qn[:, part], kn[:, part], vb[:, part])
    if stop < 1:
        x1_ref[...] = win
        return

    tail_lane = lax.broadcasted_iota(jnp.int32, (rows_q, LANES), 1)

    def scores(g, b):
        return dot(q_s[g, pl.ds(b * rows_q, rows_q), :], kbig_s[g])

    def finish(g, b, s_ref):
        factors = [scale_ref[g * heads + h] * LOG2E for h in range(heads)]
        tops, es = [], []
        for h in range(heads):
            tiles = [s_ref[:, h * main + t * LANES : h * main + (t + 1) * LANES] for t in range(main // LANES)]
            if rest:
                t = h // per_tile
                tile = s_ref[:, heads * main + t * LANES : heads * main + (t + 1) * LANES]
                tiles.append(jnp.where(tail_lane // rest == h % per_tile, tile, -3e38))
            top = functools.reduce(jnp.maximum, tiles)
            tops.append(jnp.max(top, axis=1, keepdims=True))
        for h in range(heads):
            e = jnp.exp2((s_ref[:, h * main : (h + 1) * main] - tops[h]) * factors[h])
            es.append(e.astype(jnp.bfloat16))
        if rest:
            for t in range(heads // per_tile):
                top = jnp.broadcast_to(tops[t * per_tile], (rows_q, LANES))
                factor = jnp.full((rows_q, LANES), factors[t * per_tile], jnp.float32)
                for j in range(1, per_tile):
                    top = jnp.where(tail_lane // rest == j, tops[t * per_tile + j], top)
                    factor = jnp.where(tail_lane // rest == j, factors[t * per_tile + j], factor)
                tile = s_ref[:, heads * main + t * LANES : heads * main + (t + 1) * LANES]
                es.append(jnp.exp2((tile - top) * factor).astype(jnp.bfloat16))
        o = dot(jnp.concatenate(es, axis=1), vbig_s[g])
        col = g * LANES if isinstance(g, int) else pl.multiple_of(g * LANES, LANES)
        att_s[b * rows_q : (b + 1) * rows_q, pl.ds(col, LANES)] = (o[:, :LANES] / o[:, LANES:]).astype(jnp.bfloat16)

    blocks = count // rows_q
    bufs = [sa_s, sb_s]
    sa_s[...] = scores(0, 0)
    if unroll:
        work = [(g, b) for g in range(groups) for b in range(blocks)]
        for i, (g, b) in enumerate(work):
            if i + 1 < len(work):
                bufs[(i + 1) % 2][...] = scores(*work[i + 1])
            finish(g, b, bufs[i % 2])
    else:
        def step(g, carry):
            for b in range(blocks):
                nxt = (g, b + 1) if b + 1 < blocks else (jnp.minimum(g + 1, groups - 1), 0)
                bufs[(b + 1) % 2][...] = scores(*nxt)
                finish(g, b, bufs[b % 2])
            return carry

        lax.fori_loop(0, groups, step, 0)
    if stop < 2:
        x1_ref[...] = att_s[...]
        return

    out = dot(att_s[...], wproj_ref[...])
    mean = jnp.mean(out, axis=1, keepdims=True)
    cent = out - mean
    var = jnp.mean(cent * cent, axis=1, keepdims=True)
    x1 = (win.astype(jnp.float32) + cent * lax.rsqrt(var + 1e-05) * gain_ref[...]).astype(jnp.bfloat16)
    x1_ref[...] = x1

    if stop < 3:
        return
    target = target_ref[...]
    copies, base = [], 0
    for i, sent_ref in enumerate(sent_refs):
        rows = sent_ref.shape[0]
        slot = base + lax.broadcasted_iota(jnp.int32, (rows, count), 0)
        pick = jnp.where(slot == target, 1.0, 0.0).astype(jnp.bfloat16)
        out_s[base : base + rows, :] = dot(pick, x1).astype(jnp.bfloat16)
        copies.append(pltpu.make_async_copy(out_s.at[pl.ds(base, rows)], sent_ref, sem.at[i]))
        copies[-1].start()
        base += rows
    for copy in copies:
        copy.wait()


def call_attn(first, head_scale, rolled, qkv, proj, gain, target, *, grid_rc, edge, sizes, rows_q=None, stop=9, unroll=1):
    count, feature = rolled.shape
    rows_q = rows_q or count // 2
    head_dim = feature // head_scale.shape[0]
    groups = feature // LANES
    return pl.pallas_call(
        functools.partial(attn_kernel, grid_rc, head_dim, edge, rows_q, stop, unroll),
        out_shape=(
            jax.ShapeDtypeStruct((count, feature), jnp.bfloat16),
            *[pltpu.HBM((rows, feature), jnp.bfloat16) for rows in sizes],
        ),
        in_specs=[SM, SM, VM, VM, VM, VM, VM],
        out_specs=(VM, *[HB] * len(sizes)),
        scratch_shapes=[
            pltpu.VMEM((groups, count, 2 * LANES), jnp.bfloat16),
            pltpu.VMEM((count, feature), jnp.bfloat16),
            pltpu.VMEM((groups, 2 * LANES, LANES // head_dim * count), jnp.bfloat16),
            pltpu.VMEM((groups, LANES // head_dim * count, 2 * LANES), jnp.bfloat16),
            pltpu.VMEM((rows_q, LANES // head_dim * count), jnp.float32),
            pltpu.VMEM((rows_q, LANES // head_dim * count), jnp.float32),
            pltpu.VMEM((sum(sizes), feature), jnp.bfloat16),
            pltpu.SemaphoreType.DMA((len(sizes),)),
        ],
        compiler_params=pltpu.CompilerParams(vmem_limit_bytes=32 * 1024 * 1024),
        name="attention",
    )(first, head_scale, rolled, qkv, proj, gain, target)


def expert_kernel(parts, pieces, row_block, x_ref, *refs):
    w_in, w_out, y_ref = refs[:parts], refs[parts : 2 * parts], refs[2 * parts]
    in_s, out_s, sem = refs[2 * parts + 1 :]
    feature, hidden = w_in[0].shape
    deep, wide = feature // pieces, hidden // pieces
    ins, outs = [], []
    for n in range(parts):
        for i in range(pieces):
            k = 2 * (n * pieces + i)
            rows = pl.ds(i * deep, deep)
            if n:
                ins.append(pltpu.make_async_copy(w_in[n].at[rows], in_s.at[rows, pl.ds((n - 1) * hidden, hidden)], sem.at[k]))
            outs.append(
                pltpu.make_async_copy(
                    w_out[n].at[pl.ds(i * wide, wide)], out_s.at[pl.ds(n * hidden + i * wide, wide)], sem.at[k + 1]
                )
            )
    for copy in ins + outs:
        copy.start()

    def gelu(h):
        return (0.5 * h * (1.0 + lax.erf(h * 0.7071067811865476))).astype(jnp.bfloat16)

    blocks = [slice(at, at + row_block) for at in range(0, x_ref.shape[0], row_block)]
    own = [gelu(dot(x_ref[block, :], w_in[0][...])) for block in blocks]
    for copy in ins + outs:
        copy.wait()
    for block, h in zip(blocks, own):
        h = jnp.concatenate([h, gelu(dot(x_ref[block, :], in_s[...]))], axis=1)
        y_ref[block, :] = dot(h, out_s[...]).astype(jnp.bfloat16)


def gate_kernel(x1_ref, router_ref, target_ref, ids_ref, pick_ref, scaled_ref):
    count, slots = pick_ref.shape
    target = target_ref[...]
    slot = lax.broadcasted_iota(jnp.int32, (count, slots), 1)
    pick_ref[...] = jnp.where(slot == target, 1.0, 0.0).astype(jnp.bfloat16)
    logits = dot(x1_ref[...], router_ref[...])
    mine = lax.broadcasted_iota(jnp.int32, logits.shape, 1) == ids_ref[...]
    logit = jnp.sum(jnp.where(mine, logits, 0.0), axis=1, keepdims=True)
    scaled_ref[...] = jnp.where(target < slots, jax.nn.sigmoid(logit), 0.0)


def combine_kernel(row_block, x1_ref, pick_ref, scaled_ref, gain_ref, *refs):
    *back_refs, out_ref = refs
    for i in range(x1_ref.shape[0] // row_block):
        at = slice(i * row_block, (i + 1) * row_block)
        y, base = None, 0
        for back_ref in back_refs:
            rows = back_ref.shape[0]
            term = dot(pick_ref[at, base : base + rows], back_ref[...])
            y = term if y is None else y + term
            base += rows
        mean = jnp.mean(y, axis=1, keepdims=True)
        cent = y - mean
        var = jnp.mean(cent * cent, axis=1, keepdims=True)
        add = scaled_ref[at, :] * (cent * lax.rsqrt(var + 1e-05) * gain_ref[...])
        out_ref[at, :] = (x1_ref[at, :].astype(jnp.float32) + add).astype(jnp.bfloat16)


def params(mib):
    return pltpu.CompilerParams(vmem_limit_bytes=mib * 1024 * 1024)


def body(
    tokens,
    qkv_weight,
    proj_weight,
    head_scale,
    attn_gain,
    router,
    expert_in,
    expert_out,
    moe_gain,
    expert_ids,
    keep,
):
    tile_rows, edge, feature = tokens.shape
    shift = edge // 2
    tall = lax.axis_size("tall")
    count = tile_rows * edge

    column_part = shifted(tokens[:, :shift], "wide", -1)
    widened = jnp.concatenate([tokens[:, shift:], column_part], axis=1)
    row_part = shifted(widened[:shift], "tall", -1)
    rolled = jnp.concatenate([widened[shift:], row_part], axis=0).reshape(count, feature)

    w_in = [expert_in[0]] + [shifted(expert_in[0], "tall", -n) for n in range(1, tall)]
    w_out = [expert_out[0]] + [shifted(expert_out[0], "tall", -n) for n in range(1, tall)]

    total_rows = tile_rows * tall
    total_cols = edge * lax.axis_size("wide")
    first = jnp.stack([lax.axis_index("tall") * tile_rows, lax.axis_index("wide") * edge]).astype(jnp.int32)

    route_ids = expert_ids[0, 0, :, 0]
    keep_flag = keep[0, 0]
    experts = router.shape[1]
    capacity = max(2, 3 * count // (2 * experts))
    room = -(-capacity // 8) * 8
    onehot = (route_ids[:, None] == jnp.arange(experts, dtype=jnp.int32)[None, :]).astype(jnp.int32)
    live_hits = onehot * keep_flag[:, None]
    before = jnp.cumsum(live_hits, axis=0) - live_hits
    slot_ids = jnp.sum(before * onehot, axis=1)
    parts = chunk_sizes(room)
    slots = experts * room
    row, start = jnp.zeros_like(slot_ids), 0
    for part in parts:
        here = experts * start + route_ids * part + slot_ids - start
        row = jnp.where((slot_ids >= start) & (slot_ids < start + part), here, row)
        start += part
    target = jnp.where(keep_flag == 1, row, slots)

    x1, *sent = call_attn(
        first,
        head_scale,
        rolled,
        qkv_weight,
        proj_weight,
        attn_gain[None, :],
        target[None, :],
        grid_rc=(total_rows, total_cols, shift),
        edge=edge,
        sizes=tuple(experts * part for part in parts),
    )
    hidden = w_in[0].shape[1]
    weights = w_in[:1] + [pltpu.with_memory_space_constraint(w, pltpu.HBM) for w in w_in[1:] + w_out]

    def exchange(value):
        rows = value.shape[0]
        value = value.reshape(experts, rows // experts, feature)
        return lax.all_to_all(value, "wide", split_axis=0, concat_axis=0, tiled=True).reshape(rows, feature)

    def run_experts(value):
        rows = value.shape[0]
        return pl.pallas_call(
            functools.partial(expert_kernel, tall, max(1, 4 // tall), rows // 2 if rows > 512 else rows),
            out_shape=pltpu.HBM((rows, feature), jnp.bfloat16),
            in_specs=[VM] * 2 + [HB] * (2 * tall - 1),
            out_specs=VM,
            scratch_shapes=[
                pltpu.VMEM((feature, (tall - 1) * hidden), jnp.bfloat16),
                pltpu.VMEM((tall * hidden, feature), jnp.bfloat16),
                pltpu.SemaphoreType.DMA((2 * tall * max(1, 4 // tall),)),
            ],
            compiler_params=params(32),
            cost_estimate=pl.CostEstimate(
                flops=4 * rows * feature * hidden * tall, bytes_accessed=4 * feature * hidden * tall, transcendentals=0
            ),
        )(value, *weights)

    arrived = []
    for value in sent:
        arrived.append(exchange(value))
    returned = []
    for value in arrived:
        made = run_experts(value)
        returned.append(exchange(made))

    pick, scaled = pl.pallas_call(
        gate_kernel,
        out_shape=(
            jax.ShapeDtypeStruct((count, slots), jnp.bfloat16),
            jax.ShapeDtypeStruct((count, 1), jnp.float32),
        ),
        in_specs=[VM] * 4,
        out_specs=(VM, VM),
        compiler_params=params(16),
        name="gate",
    )(x1, router, target[:, None], route_ids[:, None])
    result = pl.pallas_call(
        functools.partial(combine_kernel, count // 2),
        out_shape=jax.ShapeDtypeStruct((count, feature), jnp.bfloat16),
        in_specs=[VM] * (4 + len(parts)),
        out_specs=VM,
        compiler_params=params(16),
        name="combine",
    )(x1, pick, scaled, moe_gain[None, :], *returned)
    return result.reshape(tile_rows, edge, feature)


def solution(mesh):
    placed = (
        P("tall", "wide", None),
        P(),
        P(),
        P(),
        P(),
        P(),
        P("wide", None, "tall"),
        P("wide", "tall", None),
        P(),
        P("tall", "wide", None, None),
        P("tall", "wide", None),
    )
    return jax.shard_map(
        body, mesh=mesh, in_specs=placed, out_specs=P("tall", "wide", None), check_vma=False
    )
```
